64 devices in a mesh: dp: 8 (over x, y, core), sp: 8 (over z).
Axes of the slice: x: 2, y: 2, z: 8, core: 2. Of those that a mesh axis runs over, the one named last changes fastest.
The devices are a block of a 4x4x8 slice.
Arguments:
- x: bfloat16 [16384, 7168], P(('dp', 'sp')), parts along dimension 0
- gain: bfloat16 [7168], replicated
- wq: bfloat16 [7168, 7168], replicated
- wk: bfloat16 [7168, 1024], replicated
- wv: bfloat16 [7168, 1024], replicated
- wo: bfloat16 [7168, 7168], replicated
Outputs:
- output: bfloat16 [16384, 7168], P(('dp', 'sp')), parts along dimension 0
There are 8 independent parts. The reference program is written for one: setup_inputs(seed, part) draws one part's arguments, and reference() takes and returns one part's arrays. A program takes and returns all parts, laid end to end along the dimension named above; an argument that names none is the same for every part.
All inputs are finite; a program needn't handle non-finite values.
Results may differ from the reference program's by a relative error of at most 0.012.
Values are sent between devices in bfloat16 or wider.
A program may use at most 768 MiB of HBM per device.

```python
import jax
import jax.numpy as jnp
from jax import lax

ROWS = 2048
D = 7168
HEADS = 56
KV_HEADS = 8
HEAD = 128
THETA = 10000


def setup_inputs(seed: int = 0, part: int = 0) -> dict:
    kx, kn, kq, kk, kv, ko = jax.random.split(jax.random.key(seed), 6)

    def weights(key, rows, columns):
        return jax.random.normal(key, (rows, columns), jnp.float32) * rows**-0.5

    drawn = {
        "x": jax.random.normal(jax.random.fold_in(kx, part), (ROWS, D), jnp.float32),
        "gain": 1 + 0.1 * jax.random.normal(kn, (D,), jnp.float32),
        "wq": 2 * weights(kq, D, HEADS * HEAD),
        "wk": 2 * weights(kk, D, KV_HEADS * HEAD),
        "wv": 4 * weights(kv, D, KV_HEADS * HEAD),
        "wo": weights(ko, HEADS * HEAD, D),
    }
    return {k: v.astype(jnp.bfloat16) for k, v in drawn.items()}


def normed(x, gain):
    wide = x.astype(jnp.float32)
    scale = lax.rsqrt(jnp.mean(wide * wide, -1, keepdims=True) + 1e-6)
    return (wide * scale * gain.astype(jnp.float32)).astype(jnp.bfloat16)


def turned(t, place, theta):
    half = t.shape[-1] // 2
    angle = place.astype(jnp.float32)[:, None] * theta ** (-jnp.arange(half, dtype=jnp.float32) / half)
    cos, sin = jnp.cos(angle)[:, None], jnp.sin(angle)[:, None]
    a, b = t[..., :half].astype(jnp.float32), t[..., half:].astype(jnp.float32)
    return jnp.concatenate([a * cos - b * sin, b * cos + a * sin], -1).astype(jnp.bfloat16)


def matmul(a, w):
    return jnp.dot(a, w, preferred_element_type=jnp.float32).astype(jnp.bfloat16)


def einsum(form, a, b):
    return jnp.einsum(form, a.astype(jnp.float32), b.astype(jnp.float32))


def attention(q, k, v):
    scores = einsum("tgsd,ugd->gstu", q, k) * q.shape[-1] ** -0.5
    token = jnp.arange(q.shape[0])
    scores = jnp.where(token[:, None] >= token, scores, -jnp.inf)
    weights = jax.nn.softmax(scores, -1).astype(jnp.bfloat16)
    return einsum("gstu,ugd->tgsd", weights, v).astype(jnp.bfloat16)


def reference(x, gain, wq, wk, wv, wo):
    a, place = normed(x, gain), jnp.arange(ROWS)
    q = turned(matmul(a, wq).reshape(ROWS, HEADS, HEAD), place, THETA).reshape(ROWS, KV_HEADS, -1, HEAD)
    k = turned(matmul(a, wk).reshape(ROWS, KV_HEADS, HEAD), place, THETA)
    v = matmul(a, wv).reshape(ROWS, KV_HEADS, HEAD)
    seen = attention(q, k, v).reshape(ROWS, HEADS * HEAD)
    return (x.astype(jnp.float32) + jnp.dot(seen, wo, preferred_element_type=jnp.float32)).astype(jnp.bfloat16)
```

```python
import functools
import math

import jax
import jax.numpy as jnp
from jax import lax
from jax.experimental import pallas as pl
from jax.experimental.pallas import tpu as pltpu
from jax.sharding import PartitionSpec as P

MESH = pl.DeviceIdType.MESH
HEAD = 128
THETA = 10000
HIDDEN = -1e30
E = HEAD**-0.5 * math.log2(math.e)
VMEM = 63 * 2**20
WIDE = 256
SLOTS = 6
F32, BF16 = jnp.float32, jnp.bfloat16


def _dot(a, b, ca, cb):
    return lax.dot_general(a, b, (((ca,), (cb,)), ((), ())), preferred_element_type=F32)


def kernel(n, x_hbm, gain_ref, cos_ref, sin_ref, wk_hbm, wv_hbm, wq_hbm, wo_hbm, out_ref,
           a_s, y_s, q_s, o_s, kv_s, s_s, m_s, w_s, w_sem, x_sem, send_sem, recv_sem):
    me = lax.axis_index("sp")
    right, left = lax.rem(me + 1, n), lax.rem(me + n - 1, n)
    own, d = x_hbm.shape
    kv_heads = wk_hbm.shape[1] // HEAD
    heads = wq_hbm.shape[1] // HEAD
    group = heads // kv_heads
    pairs = kv_heads // 2
    run = 2 * group
    deep = run * HEAD
    part = d // deep
    kv_tiles, q_tiles = 2 * pairs, heads // 2
    o_tiles = wo_hbm.shape[1] // (WIDE * part)
    tiles = kv_tiles + q_tiles + pairs * o_tiles

    def fetch(u):
        slot = lax.rem(u, SLOTS)
        sem = w_sem.at[slot]

        def columns(w, i):
            cols = pl.ds(pl.multiple_of(i * WIDE, WIDE), WIDE)
            pltpu.make_async_copy(w.at[:, cols], w_s.at[slot], sem).start()

        @pl.when((u < kv_tiles) & (lax.rem(u, 2) == 0))
        def _():
            columns(wk_hbm, lax.div(u, 2))

        @pl.when((u < kv_tiles) & (lax.rem(u, 2) == 1))
        def _():
            columns(wv_hbm, lax.div(u, 2))

        @pl.when((u >= kv_tiles) & (u < kv_tiles + q_tiles))
        def _():
            columns(wq_hbm, u - kv_tiles)

        @pl.when((u >= kv_tiles + q_tiles) & (u < tiles))
        def _():
            i = u - kv_tiles - q_tiles
            c, t = lax.div(i, o_tiles), lax.rem(i, o_tiles)
            rows = pl.ds(pl.multiple_of(c * deep, deep), deep)
            for j in range(part):
                cols = pl.ds(pl.multiple_of((t * part + j) * WIDE, WIDE), WIDE)
                pltpu.make_async_copy(wo_hbm.at[rows, cols], w_s.at[slot, pl.ds(j * deep, deep), :], sem).start()

    def arrived(u):
        slot = lax.rem(u, SLOTS)
        pltpu.make_async_copy(wq_hbm.at[:, pl.ds(0, WIDE)], w_s.at[slot], w_sem.at[slot]).wait()
        fetch(u + SLOTS - 1)
        return slot

    def message(c, s, way):
        second = lax.rem(s, 2) if way == 0 else 1 - lax.rem(s, 2)
        hop = lax.div(s, 2)
        head = 2 * c + second
        if way == 0:
            block = me - hop
            valid = (block >= 0) & (me < n - 1)
            to = right
        else:
            block = lax.rem(me + hop, n)
            valid = block < n - 1 - n // 2 + second
            to = left
        here = kv_s.at[head, jnp.maximum(block, 0)]
        copy = pltpu.make_async_remote_copy(
            src_ref=here, dst_ref=here, send_sem=send_sem.at[way, head, hop], recv_sem=recv_sem.at[head, jnp.maximum(block, 0)],
            device_id={"sp": to}, device_id_type=MESH)
        return copy, valid, hop

    def tick(c, s):
        for way in (0, 1):
            copy, valid, hop = message(c, s, way)

            @pl.when(valid & (hop > 0))
            def _():
                copy.wait_recv()

            @pl.when(valid)
            def _():
                copy.start()

    hops = n - 1

    pltpu.make_async_copy(x_hbm, out_ref, x_sem).start()
    for u in range(SLOTS - 1):
        fetch(jnp.int32(u))
    barrier = pltpu.get_barrier_semaphore()
    for neighbour in (left, right):
        pl.semaphore_signal(barrier, inc=1, device_id={"sp": neighbour}, device_id_type=MESH)
    pl.semaphore_wait(barrier, 2)
    pltpu.make_async_copy(x_hbm, out_ref, x_sem).wait()

    def norm(i, _):
        rows = pl.ds(pl.multiple_of(i * 16, 16), 16)
        wide = out_ref[rows, :].astype(F32)
        y_s[rows, :] = wide
        scale = lax.rsqrt(jnp.mean(wide * wide, -1, keepdims=True) + 1e-6)
        a_s[rows, :] = (wide * scale * gain_ref[...]).astype(BF16)

    lax.fori_loop(0, own // 16, norm, None)

    def turned(t):
        t = t.astype(BF16).astype(F32)
        return (t * cos_ref[...] + pltpu.roll(t, HEAD // 2, 1) * sin_ref[...]).astype(BF16)

    def keys_values(p, _):
        slot = arrived(2 * p)
        k = _dot(a_s[...], w_s[slot], 1, 0)
        for i in range(2):
            kv_s[2 * p + i, me, :own, :] = turned(k[:, i * HEAD : (i + 1) * HEAD])
        slot = arrived(2 * p + 1)
        v = _dot(a_s[...], w_s[slot], 1, 0)
        for i in range(2):
            vt = v[:, i * HEAD : (i + 1) * HEAD].T.astype(BF16)
            for j in range(own // HEAD):
                kv_s[2 * p + i, me, own + j * HEAD : own + (j + 1) * HEAD, :] = vt[:, j * HEAD : (j + 1) * HEAD]
        tick(0, p)

    lax.fori_loop(0, pairs, keys_values, None)

    spare = 2 * hops - pairs

    def queries(i, _):
        slot = arrived(kv_tiles + i)
        q = _dot(a_s[...], w_s[slot], 1, 0)
        for j in range(2):
            q_s[2 * i + j] = turned(q[:, j * HEAD : (j + 1) * HEAD])
        done, now = lax.div(i * spare, q_tiles), lax.div((i + 1) * spare, q_tiles)

        @pl.when(now > done)
        def _():
            s = done + pairs
            tick(lax.div(s, hops), lax.rem(s, hops))

    lax.fori_loop(0, q_tiles, queries, None)

    def attend(c, blocks):
        keys = blocks * own
        at = blocks - 1
        for second in range(2):
            far, back = n // 2 - second, n - 1 - n // 2 + second
            for b in range(at):
                ahead = at - b
                passed_on = (ahead < far and at < n - 1) if ahead <= far else n - ahead < back
                if not passed_on:
                    pltpu.make_async_copy(kv_s.at[2 * c + second, b], kv_s.at[2 * c + second, b], recv_sem.at[2 * c + second, b]).wait()

        def scores(slot, h):
            k = kv_s[2 * c + lax.div(h, group), :blocks, :own, :].reshape(keys, HEAD)
            s = _dot(k, q_s[c * run + h], 1, 1)
            last = s[keys - own :]
            seen = lax.broadcasted_iota(jnp.int32, last.shape, 0) <= lax.broadcasted_iota(jnp.int32, last.shape, 1)
            last = jnp.where(seen, last, HIDDEN)
            top = last.max(axis=0, keepdims=True)
            if blocks > 1:
                s_s[slot, : keys - own] = s[: keys - own]
                top = jnp.maximum(top, s[: keys - own].max(axis=0, keepdims=True))
            s_s[slot, keys - own : keys] = last
            m_s[slot] = top * E

        def values(slot, h):
            p = jnp.exp2(s_s[slot, :keys] * E - m_s[slot]).astype(BF16)
            g = 2 * c + lax.div(h, group)
            vt = [kv_s[g, b, own + j * HEAD : own + (j + 1) * HEAD, :] for b in range(blocks) for j in range(own // HEAD)]
            vt = jnp.concatenate([jnp.concatenate(vt, axis=1), jnp.ones((16, keys), BF16)], axis=0)
            o = _dot(vt, p, 1, 0)
            o = (o[:HEAD] * (1 / o[HEAD : HEAD + 1])).T.astype(BF16)
            o_s[:, pl.ds(pl.multiple_of(h * HEAD, HEAD), HEAD)] = o

        scores(0, jnp.int32(0))

        def two(i, _):
            h = 2 * i
            scores(1, h + 1)
            values(0, h)
            scores(0, jnp.minimum(h + 2, run - 1))
            values(1, h + 1)

            @pl.when((lax.rem(i, 2) == 1) & (c < pairs - 2))
            def _():
                tick(c + 2, lax.div(i, 2))

        lax.fori_loop(0, run // 2, two, None)

    def a_run(c, _):
        for blocks in range(1, n + 1):
            pl.when(me == blocks - 1)(functools.partial(attend, c, blocks))

        def project(t, _):
            slot = arrived(kv_tiles + q_tiles + c * o_tiles + t)
            for j in range(part):
                cols = pl.ds(pl.multiple_of((t * part + j) * WIDE, WIDE), WIDE)
                y_s[:, cols] = y_s[:, cols] + _dot(o_s[...], w_s[slot, j * deep : (j + 1) * deep, :], 1, 0)

            @pl.when(c == pairs - 1)
            def _():
                cols = pl.ds(pl.multiple_of(t * part * WIDE, WIDE), part * WIDE)
                out_ref[:, cols] = y_s[:, cols].astype(BF16)

            @pl.when((lax.rem(t, 2) == 0) & (c < pairs - 2))
            def _():
                tick(c + 2, run // 4 + lax.div(t, 2))

        lax.fori_loop(0, o_tiles, project, None)

    lax.fori_loop(0, pairs, a_run, None)

    def sent(i, _):
        for way in (0, 1):
            copy, valid, _ = message(lax.div(i, hops), lax.rem(i, hops), way)
            pl.when(valid)(copy.wait_send)

    lax.fori_loop(0, pairs * hops, sent, None)


def solution(mesh):
    n = mesh.shape["sp"]

    def step(x, gain, wq, wk, wv, wo):
        own, d = x.shape
        half = HEAD // 2
        kv_heads, heads = wk.shape[1] // HEAD, wq.shape[1] // HEAD
        run = 2 * heads // kv_heads
        place = (lax.axis_index("sp") * own + jnp.arange(own)).astype(F32)
        angle = place[:, None] * THETA ** (-jnp.arange(half, dtype=F32) / half)
        cos, sin = jnp.cos(angle), jnp.sin(angle)
        cos, sin = jnp.concatenate([cos, cos], -1), jnp.concatenate([-sin, sin], -1)
        vmem, hbm = pl.BlockSpec(memory_space=pltpu.VMEM), pl.BlockSpec(memory_space=pl.ANY)
        return pl.pallas_call(
            functools.partial(kernel, n),
            out_shape=jax.ShapeDtypeStruct((own, d), BF16),
            in_specs=[hbm, vmem, vmem, vmem, hbm, hbm, hbm, hbm],
            out_specs=vmem,
            scratch_shapes=[
                pltpu.VMEM((own, d), BF16),
                pltpu.VMEM((own, d), F32),
                pltpu.VMEM((heads, own, HEAD), BF16),
                pltpu.VMEM((own, run * HEAD), BF16),
                pltpu.VMEM((kv_heads, n, 2 * own, HEAD), BF16),
                pltpu.VMEM((2, n * own, own), F32),
                pltpu.VMEM((2, 1, own), F32),
                pltpu.VMEM((SLOTS, d, WIDE), BF16),
                pltpu.SemaphoreType.DMA((SLOTS,)),
                pltpu.SemaphoreType.DMA,
                pltpu.SemaphoreType.DMA((2, kv_heads, n // 2)),
                pltpu.SemaphoreType.DMA((kv_heads, n)),
            ],
            compiler_params=pltpu.CompilerParams(collective_id=0, has_side_effects=True, vmem_limit_bytes=VMEM),
        )(x, gain.astype(F32)[None], cos, sin, wk, wv, wq, wo)

    tokens, whole = P(("dp", "sp"), None), P(None, None)
    return jax.shard_map(
        step,
        mesh=mesh,
        in_specs=(tokens, P(None), whole, whole, whole, whole),
        out_specs=tokens,
        check_vma=False,
    )
```

```python
import functools
import math

import jax
import jax.numpy as jnp
import numpy as np
from jax import lax
from jax.experimental import pallas as pl
from jax.experimental.pallas import tpu as pltpu
from jax.sharding import PartitionSpec as P

MESH = pl.DeviceIdType.MESH
HEAD = 128
THETA = 10000
HIDDEN = -1e30
E = HEAD**-0.5 * math.log2(math.e)
VMEM = 67_043_328
WIDE = 256
SLOTS = 8
F32, BF16 = jnp.float32, jnp.bfloat16


def _dot(a, b, ca, cb):
    return lax.dot_general(a, b, (((ca,), (cb,)), ((), ())), preferred_element_type=F32)


def kernel(n, x_hbm, gain_ref, turn_ref, wk_hbm, wv_hbm, wq_hbm, wo_hbm, out_ref,
           a_s, y_s, q_s, o_s, kv_s, s_s, m_s, cos_s, sin_s, w_s, w_sem, x_sem, send_sem, recv_sem):
    me = lax.axis_index("sp")
    right, left = lax.rem(me + 1, n), lax.rem(me + n - 1, n)
    own, d = x_hbm.shape
    kv_heads = wk_hbm.shape[1] // HEAD
    heads = wq_hbm.shape[1] // HEAD
    group = heads // kv_heads
    pairs = kv_heads // 2
    runs = pairs // 2
    run = 4 * group
    deep = run * HEAD
    part = d // deep
    kv_tiles, q_tiles = 2 * pairs, heads // 2
    o_tiles = wo_hbm.shape[1] // (WIDE * part)
    tiles = kv_tiles + q_tiles + runs * o_tiles

    def fetch(u):
        slot = lax.rem(u, SLOTS)
        sem = w_sem.at[slot]

        def columns(w, i):
            cols = pl.ds(pl.multiple_of(i * WIDE, WIDE), WIDE)
            pltpu.make_async_copy(w.at[:, cols], w_s.at[slot], sem).start()

        @pl.when((u < kv_tiles) & (lax.rem(u, 2) == 0))
        def _():
            columns(wk_hbm, lax.div(u, 2))

        @pl.when((u < kv_tiles) & (lax.rem(u, 2) == 1))
        def _():
            columns(wv_hbm, lax.div(u, 2))

        @pl.when((u >= kv_tiles) & (u < kv_tiles + q_tiles))
        def _():
            columns(wq_hbm, u - kv_tiles)

        @pl.when((u >= kv_tiles + q_tiles) & (u < tiles))
        def _():
            i = u - kv_tiles - q_tiles
            c, t = lax.div(i, o_tiles), lax.rem(i, o_tiles)
            rows = pl.ds(pl.multiple_of(c * deep, deep), deep)
            for j in range(part):
                cols = pl.ds(pl.multiple_of((t * part + j) * WIDE, WIDE), WIDE)
                pltpu.make_async_copy(wo_hbm.at[rows, cols], w_s.at[slot, pl.ds(j * deep, deep), :], sem).start()

    def arrived(u):
        for i in range(2):
            fetch(u + SLOTS - 2 + i)
        slots = [lax.rem(u + i, SLOTS) for i in range(2)]
        for slot in slots:
            pltpu.make_async_copy(wq_hbm.at[:, pl.ds(0, WIDE)], w_s.at[slot], w_sem.at[slot]).wait()
        return slots

    def message(c, s, way):
        second = lax.rem(s, 2) if way == 0 else 1 - lax.rem(s, 2)
        hop = lax.div(s, 2)
        head = 2 * c + second
        if way == 0:
            block = me - hop
            valid = (block >= 0) & (me < n - 1)
            to = right
        else:
            block = lax.rem(me + hop, n)
            valid = block < n - 1 - n // 2 + second
            to = left
        here = kv_s.at[head, jnp.maximum(block, 0)]
        copy = pltpu.make_async_remote_copy(
            src_ref=here, dst_ref=here, send_sem=send_sem.at[way, head, hop], recv_sem=recv_sem.at[head, jnp.maximum(block, 0)],
            device_id={"sp": to}, device_id_type=MESH)
        return copy, valid, hop

    hops = n - 1

    def tick(m):
        for way in (0, 1):
            copy, valid, hop = message(lax.div(m, hops), lax.rem(m, hops), way)

            @pl.when(valid & (hop > 0))
            def _():
                copy.wait_recv()

            @pl.when(valid)
            def _():
                copy.start()

    def ticks(first, end, step, steps):
        before, after = lax.div(step * (end - first), steps), lax.div((step + 1) * (end - first), steps)

        @pl.when(after > before)
        def _():
            tick(first + before)

    last = pairs * hops
    by_queries, by_first = last // 2 + 1, last - 3

    pltpu.make_async_copy(x_hbm, out_ref, x_sem).start()
    barrier = pltpu.get_barrier_semaphore()
    for neighbour in (left, right):
        pl.semaphore_signal(barrier, inc=1, device_id={"sp": neighbour}, device_id_type=MESH)
    place = (me * own + lax.broadcasted_iota(jnp.int32, (own, HEAD), 0)).astype(F32)
    angle = place * turn_ref[...]
    cos_s[...] = jnp.cos(angle)
    sin = jnp.sin(angle)
    sin_s[...] = jnp.where(lax.broadcasted_iota(jnp.int32, (own, HEAD), 1) < HEAD // 2, -sin, sin)
    pl.semaphore_wait(barrier, 2)
    pltpu.make_async_copy(x_hbm, out_ref, x_sem).wait()
    for u in range(2):
        fetch(jnp.int32(u))

    def norm(i, _):
        rows = pl.ds(pl.multiple_of(i * 16, 16), 16)
        wide = out_ref[rows, :].astype(F32)
        y_s[rows, :] = wide
        scale = lax.rsqrt(jnp.mean(wide * wide, -1, keepdims=True) + 1e-6)
        a_s[rows, :] = (wide * scale * gain_ref[...]).astype(BF16)

    stages = SLOTS - 4
    for j in range(stages):
        lax.fori_loop(j * own // 16 // stages, (j + 1) * own // 16 // stages, norm, None)
        fetch(jnp.int32(2 + j))

    def turned(t):
        t = t.astype(BF16).astype(F32)
        return (t * cos_s[...] + pltpu.roll(t, HEAD // 2, 1) * sin_s[...]).astype(BF16)

    def keys_values(p, _):
        of_k, of_v = arrived(2 * p)
        k = _dot(a_s[...], w_s[of_k], 1, 0)
        v = _dot(a_s[...], w_s[of_v], 1, 0)
        for i in range(2):
            kv_s[2 * p + i, me, :own, :] = turned(k[:, i * HEAD : (i + 1) * HEAD])
            vt = v[:, i * HEAD : (i + 1) * HEAD].T.astype(BF16)
            for j in range(own // HEAD):
                kv_s[2 * p + i, me, own + j * HEAD : own + (j + 1) * HEAD, :] = vt[:, j * HEAD : (j + 1) * HEAD]
        tick(p)

    for u in range(2 + stages, SLOTS - 2):
        fetch(jnp.int32(u))
    lax.fori_loop(0, pairs, keys_values, None)

    def queries(i, _):
        slots = arrived(kv_tiles + 2 * i)
        both = [_dot(a_s[...], w_s[slot], 1, 0) for slot in slots]
        for t, q in enumerate(both):
            for j in range(2):
                q_s[4 * i + 2 * t + j] = turned(q[:, j * HEAD : (j + 1) * HEAD])
        ticks(pairs, by_queries, i, q_tiles // 2)

    lax.fori_loop(0, q_tiles // 2, queries, None)

    steps = run // 4

    def attend(c, blocks):
        keys = blocks * own
        at = blocks - 1

        def landed(pair):
            for second in range(2):
                far, back = n // 2 - second, n - 1 - n // 2 + second
                for b in range(at):
                    ahead = at - b
                    passed_on = (ahead < far and at < n - 1) if ahead <= far else n - ahead < back
                    if not passed_on:
                        here = kv_s.at[2 * pair + second, b]
                        pltpu.make_async_copy(here, here, recv_sem.at[2 * pair + second, b]).wait()

        def scores(slot, h):
            k = kv_s[4 * c + lax.div(h, group), :blocks, :own, :].reshape(keys, HEAD)
            s = _dot(k, q_s[c * run + h], 1, 1)
            near = s[keys - own :]
            seen = lax.broadcasted_iota(jnp.int32, near.shape, 0) <= lax.broadcasted_iota(jnp.int32, near.shape, 1)
            near = jnp.where(seen, near, HIDDEN)
            top = near.max(axis=0, keepdims=True)
            if blocks > 1:
                s_s[slot, : keys - own] = s[: keys - own]
                top = jnp.maximum(top, s[: keys - own].max(axis=0, keepdims=True))
            s_s[slot, keys - own : keys] = near
            m_s[slot] = top * E

        def values(slot, h):
            p = jnp.exp2(s_s[slot, :keys] * E - m_s[slot]).astype(BF16)
            g = 4 * c + lax.div(h, group)
            vt = [kv_s[g, b, own + j * HEAD : own + (j + 1) * HEAD, :] for b in range(blocks) for j in range(own // HEAD)]
            vt = jnp.concatenate([jnp.concatenate(vt, axis=1), jnp.ones((16, keys), BF16)], axis=0)
            o = _dot(vt, p, 1, 0)
            o = (o[:HEAD] * (1 / o[HEAD : HEAD + 1])).T.astype(BF16)
            o_s[:, pl.ds(pl.multiple_of(h * HEAD, HEAD), HEAD)] = o

        landed(2 * c)
        scores(0, jnp.int32(0))

        def four(i, _):
            @pl.when(i == (2 * group - 1) // 4)
            def _():
                landed(2 * c + 1)

            for j in range(4):
                scores((j + 1) % 2, jnp.minimum(4 * i + j + 1, run - 1))
                values(j % 2, 4 * i + j)

            @pl.when(c == 0)
            def _():
                ticks(by_queries, by_first, i, 2 * steps)

            @pl.when((c == 1) & (i < last - by_first))
            def _():
                tick(by_first + i)

        lax.fori_loop(0, steps, four, None)

    def a_run(c, _):
        for blocks in range(1, n + 1):
            pl.when(me == blocks - 1)(functools.partial(attend, c, blocks))

        def project(t, _):
            slots = arrived(kv_tiles + q_tiles + c * o_tiles + 2 * t)
            for i, slot in enumerate(slots):
                for j in range(part):
                    cols = pl.ds(pl.multiple_of(((2 * t + i) * part + j) * WIDE, WIDE), WIDE)
                    y_s[:, cols] = y_s[:, cols] + _dot(o_s[...], w_s[slot, j * deep : (j + 1) * deep, :], 1, 0)

            @pl.when(c == runs - 1)
            def _():
                cols = pl.ds(pl.multiple_of(2 * t * part * WIDE, WIDE), 2 * part * WIDE)
                out_ref[:, cols] = y_s[:, cols].astype(BF16)

            @pl.when(c == 0)
            def _():
                ticks(by_queries, by_first, steps + t, 2 * steps)

        lax.fori_loop(0, o_tiles // 2, project, None)

    lax.fori_loop(0, runs, a_run, None)

    def sent(i, _):
        for way in (0, 1):
            copy, valid, _ = message(lax.div(i, hops), lax.rem(i, hops), way)
            pl.when(valid)(copy.wait_send)

    lax.fori_loop(0, pairs * hops, sent, None)


def solution(mesh):
    n = mesh.shape["sp"]

    def step(x, gain, wq, wk, wv, wo):
        own, d = x.shape
        kv_heads, heads = wk.shape[1] // HEAD, wq.shape[1] // HEAD
        run = 4 * heads // kv_heads
        half = np.arange(HEAD) % (HEAD // 2)
        turn = jnp.asarray((float(THETA) ** (-2.0 * half / HEAD)).astype(np.float32)[None])
        vmem, hbm = pl.BlockSpec(memory_space=pltpu.VMEM), pl.BlockSpec(memory_space=pl.ANY)
        return pl.pallas_call(
            functools.partial(kernel, n),
            out_shape=jax.ShapeDtypeStruct((own, d), BF16),
            in_specs=[hbm, vmem, vmem, hbm, hbm, hbm, hbm],
            out_specs=vmem,
            scratch_shapes=[
                pltpu.VMEM((own, d), BF16),
                pltpu.VMEM((own, d), F32),
                pltpu.VMEM((heads, own, HEAD), BF16),
                pltpu.VMEM((own, run * HEAD), BF16),
                pltpu.VMEM((kv_heads, n, 2 * own, HEAD), BF16),
                pltpu.VMEM((2, n * own, own), F32),
                pltpu.VMEM((2, 1, own), F32),
                pltpu.VMEM((own, HEAD), F32),
                pltpu.VMEM((own, HEAD), F32),
                pltpu.VMEM((SLOTS, d, WIDE), BF16),
                pltpu.SemaphoreType.DMA((SLOTS,)),
                pltpu.SemaphoreType.DMA,
                pltpu.SemaphoreType.DMA((2, kv_heads, n // 2)),
                pltpu.SemaphoreType.DMA((kv_heads, n)),
            ],
            compiler_params=pltpu.CompilerParams(collective_id=0, has_side_effects=True, vmem_limit_bytes=VMEM),
        )(x, gain.astype(F32)[None], turn, wk, wv, wq, wo)

    tokens, whole = P(("dp", "sp"), None), P(None, None)
    return jax.shard_map(
        step,
        mesh=mesh,
        in_specs=(tokens, P(None), whole, whole, whole, whole),
        out_specs=tokens,
        check_vma=False,
    )
```

```python
import functools
import math

import jax
import jax.numpy as jnp
import numpy as np
from jax import lax
from jax.experimental import pallas as pl
from jax.experimental.pallas import tpu as pltpu
from jax.sharding import PartitionSpec as P

MESH = pl.DeviceIdType.MESH
HEAD = 128
THETA = 10000
HIDDEN = -1e30
E = HEAD**-0.5 * math.log2(math.e)
VMEM = 67_043_328
WIDE = 256
SLOTS = 8
F32, BF16 = jnp.float32, jnp.bfloat16


def _dot(a, b, ca, cb):
    return lax.dot_general(a, b, (((ca,), (cb,)), ((), ())), preferred_element_type=F32)


def kernel(n, x_hbm, gain_ref, turn_ref, wk_hbm, wv_hbm, wq_hbm, wo_hbm, out_ref,
           a_s, y_s, q_s, o_s, kv_s, s_s, m_s, cos_s, sin_s, w_s, w_sem, x_sem, send_sem, recv_sem):
    me = lax.axis_index("sp")
    right, left = lax.rem(me + 1, n), lax.rem(me + n - 1, n)
    own, d = x_hbm.shape
    kv_heads = wk_hbm.shape[1] // HEAD
    heads = wq_hbm.shape[1] // HEAD
    group = heads // kv_heads
    pairs = kv_heads // 2
    run = 2 * group
    deep = run * HEAD
    part = d // deep
    kv_tiles, q_tiles = 2 * pairs, heads // 2
    o_tiles = wo_hbm.shape[1] // (WIDE * part)
    tiles = kv_tiles + q_tiles + pairs * o_tiles

    def fetch(u):
        slot = lax.rem(u, SLOTS)
        sem = w_sem.at[slot]

        def columns(w, i):
            cols = pl.ds(pl.multiple_of(i * WIDE, WIDE), WIDE)
            pltpu.make_async_copy(w.at[:, cols], w_s.at[slot], sem).start()

        @pl.when((u < kv_tiles) & (lax.rem(u, 2) == 0))
        def _():
            columns(wk_hbm, lax.div(u, 2))

        @pl.when((u < kv_tiles) & (lax.rem(u, 2) == 1))
        def _():
            columns(wv_hbm, lax.div(u, 2))

        @pl.when((u >= kv_tiles) & (u < kv_tiles + q_tiles))
        def _():
            columns(wq_hbm, u - kv_tiles)

        @pl.when((u >= kv_tiles + q_tiles) & (u < tiles))
        def _():
            i = u - kv_tiles - q_tiles
            c, t = lax.div(i, o_tiles), lax.rem(i, o_tiles)
            rows = pl.ds(pl.multiple_of(c * deep, deep), deep)
            for j in range(part):
                cols = pl.ds(pl.multiple_of((t * part + j) * WIDE, WIDE), WIDE)
                pltpu.make_async_copy(wo_hbm.at[rows, cols], w_s.at[slot, pl.ds(j * deep, deep), :], sem).start()

    def arrived(u, count=2):
        for i in range(count):
            fetch(u + SLOTS - 2 + i)
        slots = [lax.rem(u + i, SLOTS) for i in range(count)]
        for slot in slots:
            pltpu.make_async_copy(wq_hbm.at[:, pl.ds(0, WIDE)], w_s.at[slot], w_sem.at[slot]).wait()
        return slots

    def message(c, s, way):
        second = lax.rem(s, 2) if way == 0 else 1 - lax.rem(s, 2)
        hop = lax.div(s, 2)
        head = 2 * c + second
        if way == 0:
            block = me - hop
            valid = (block >= 0) & (me < n - 1)
            to = right
        else:
            block = lax.rem(me + hop, n)
            valid = block < n - 1 - n // 2 + second
            to = left
        here = kv_s.at[head, jnp.maximum(block, 0)]
        copy = pltpu.make_async_remote_copy(
            src_ref=here, dst_ref=here, send_sem=send_sem.at[way, head, hop], recv_sem=recv_sem.at[head, jnp.maximum(block, 0)],
            device_id={"sp": to}, device_id_type=MESH)
        return copy, valid, hop

    hops = n - 1

    def tick(m):
        for way in (0, 1):
            copy, valid, hop = message(lax.div(m, hops), lax.rem(m, hops), way)

            @pl.when(valid & (hop > 0))
            def _():
                copy.wait_recv()

            @pl.when(valid)
            def _():
                copy.start()

    def ticks(first, end, step, steps):
        before, after = lax.div(step * (end - first), steps), lax.div((step + 1) * (end - first), steps)

        @pl.when(after > before)
        def _():
            tick(first + before)

    last = pairs * hops
    by_queries = last // 2 + 1
    by_run = [by_queries + math.ceil((last - by_queries) * r / (pairs - 1)) for r in range(pairs)]

    pltpu.make_async_copy(x_hbm, out_ref, x_sem).start()
    barrier = pltpu.get_barrier_semaphore()
    for neighbour in (left, right):
        pl.semaphore_signal(barrier, inc=1, device_id={"sp": neighbour}, device_id_type=MESH)
    place = (me * own + lax.broadcasted_iota(jnp.int32, (own, HEAD), 0)).astype(F32)
    angle = place * turn_ref[...]
    cos_s[...] = jnp.cos(angle)
    sin = jnp.sin(angle)
    sin_s[...] = jnp.where(lax.broadcasted_iota(jnp.int32, (own, HEAD), 1) < HEAD // 2, -sin, sin)
    pl.semaphore_wait(barrier, 2)
    pltpu.make_async_copy(x_hbm, out_ref, x_sem).wait()
    for u in range(2):
        fetch(jnp.int32(u))

    def norm(i, _):
        rows = pl.ds(pl.multiple_of(i * 16, 16), 16)
        wide = out_ref[rows, :].astype(F32)
        y_s[rows, :] = wide
        scale = lax.rsqrt(jnp.mean(wide * wide, -1, keepdims=True) + 1e-6)
        a_s[rows, :] = (wide * scale * gain_ref[...].astype(F32)).astype(BF16)

    stages = SLOTS - 4
    for j in range(stages):
        lax.fori_loop(j * own // 16 // stages, (j + 1) * own // 16 // stages, norm, None)
        fetch(jnp.int32(2 + j))

    def turned(t):
        t = t.astype(BF16).astype(F32)
        return (t * cos_s[...] + pltpu.roll(t, HEAD // 2, 1) * sin_s[...]).astype(BF16)

    def keys_values(p, _):
        of_k, of_v = arrived(2 * p)
        k = _dot(a_s[...], w_s[of_k], 1, 0)
        v = _dot(a_s[...], w_s[of_v], 1, 0)
        for i in range(2):
            kv_s[2 * p + i, me, :own, :] = turned(k[:, i * HEAD : (i + 1) * HEAD])
            vt = v[:, i * HEAD : (i + 1) * HEAD].T.astype(BF16)
            for j in range(own // HEAD):
                kv_s[2 * p + i, me, own + j * HEAD : own + (j + 1) * HEAD, :] = vt[:, j * HEAD : (j + 1) * HEAD]
        tick(p)

    for u in range(2 + stages, SLOTS - 2):
        fetch(jnp.int32(u))
    lax.fori_loop(0, pairs, keys_values, None)

    def queries(i, _):
        slots = arrived(kv_tiles + 2 * i)
        both = [_dot(a_s[...], w_s[slot], 1, 0) for slot in slots]
        for t, q in enumerate(both):
            for j in range(2):
                q_s[4 * i + 2 * t + j] = turned(q[:, j * HEAD : (j + 1) * HEAD])
        ticks(pairs, by_queries, i, q_tiles // 2)

    lax.fori_loop(0, q_tiles // 2, queries, None)

    fours, twos = divmod(run, 4)
    doubles, singles = divmod(o_tiles, 2)
    steps = fours + (twos > 0) + doubles + singles

    def run_ticks(c, step):
        for r in range(pairs - 1):
            pl.when(c == r)(functools.partial(ticks, by_run[r], by_run[r + 1], step, steps))

    def attend(c, blocks):
        keys = blocks * own
        at = blocks - 1

        def landed(pair):
            for second in range(2):
                far, back = n // 2 - second, n - 1 - n // 2 + second
                for b in range(at):
                    ahead = at - b
                    passed_on = (ahead < far and at < n - 1) if ahead <= far else n - ahead < back
                    if not passed_on:
                        here = kv_s.at[2 * pair + second, b]
                        pltpu.make_async_copy(here, here, recv_sem.at[2 * pair + second, b]).wait()

        def scores(slot, h):
            k = kv_s[2 * c + lax.div(h, group), :blocks, :own, :].reshape(keys, HEAD)
            s = _dot(k, q_s[c * run + h], 1, 1)
            near = s[keys - own :]
            seen = lax.broadcasted_iota(jnp.int32, near.shape, 0) <= lax.broadcasted_iota(jnp.int32, near.shape, 1)
            near = jnp.where(seen, near, HIDDEN)
            top = near.max(axis=0, keepdims=True)
            if blocks > 1:
                s_s[slot, : keys - own] = s[: keys - own]
                top = jnp.maximum(top, s[: keys - own].max(axis=0, keepdims=True))
            s_s[slot, keys - own : keys] = near
            m_s[slot] = top * E

        def values(slot, h):
            p = jnp.exp2(s_s[slot, :keys] * E - m_s[slot]).astype(BF16)
            g = 2 * c + lax.div(h, group)
            vt = [kv_s[g, b, own + j * HEAD : own + (j + 1) * HEAD, :] for b in range(blocks) for j in range(own // HEAD)]
            vt = jnp.concatenate([jnp.concatenate(vt, axis=1), jnp.ones((16, keys), BF16)], axis=0)
            o = _dot(vt, p, 1, 0)
            o = (o[:HEAD] * (1 / o[HEAD : HEAD + 1])).T.astype(BF16)
            o_s[:, pl.ds(pl.multiple_of(h * HEAD, HEAD), HEAD)] = o

        landed(c)
        scores(0, jnp.int32(0))

        def some(h, count, more):
            for j in range(count):
                if j + 1 < count or more:
                    scores((j + 1) % 2, h + j + 1)
                values(j % 2, h + j)

        def four(i, _):
            some(4 * i, 4, True)
            run_ticks(c, i)

        lax.fori_loop(0, fours if twos else fours - 1, four, None)
        some(jnp.int32(run - (twos or 4)), twos or 4, False)
        run_ticks(c, fours if twos else fours - 1)

    def a_run(c, _):
        for blocks in range(1, n + 1):
            pl.when(me == blocks - 1)(functools.partial(attend, c, blocks))

        def project(t, count, step):
            slots = arrived(kv_tiles + q_tiles + c * o_tiles + t, count)
            for i, slot in enumerate(slots):
                for j in range(part):
                    cols = pl.ds(pl.multiple_of(((t + i) * part + j) * WIDE, WIDE), WIDE)
                    y_s[:, cols] = y_s[:, cols] + _dot(o_s[...], w_s[slot, j * deep : (j + 1) * deep, :], 1, 0)

            @pl.when(c == pairs - 1)
            def _():
                cols = pl.ds(pl.multiple_of(t * part * WIDE, WIDE), count * part * WIDE)
                out_ref[:, cols] = y_s[:, cols].astype(BF16)

            run_ticks(c, step)

        lax.fori_loop(0, doubles, lambda t, _: project(2 * t, 2, steps - doubles - singles + t), None)
        if singles:
            project(jnp.int32(2 * doubles), 1, steps - 1)

    lax.fori_loop(0, pairs, a_run, None)

    def sent(i, _):
        for way in (0, 1):
            copy, valid, _ = message(lax.div(i, hops), lax.rem(i, hops), way)
            pl.when(valid)(copy.wait_send)

    lax.fori_loop(0, pairs * hops, sent, None)


def solution(mesh):
    n = mesh.shape["sp"]

    def step(x, gain, wq, wk, wv, wo):
        own, d = x.shape
        kv_heads, heads = wk.shape[1] // HEAD, wq.shape[1] // HEAD
        run = 2 * heads // kv_heads
        half = np.arange(HEAD) % (HEAD // 2)
        turn = jnp.asarray((float(THETA) ** (-2.0 * half / HEAD)).astype(np.float32)[None])
        vmem, hbm = pl.BlockSpec(memory_space=pltpu.VMEM), pl.BlockSpec(memory_space=pl.ANY)
        return pl.pallas_call(
            functools.partial(kernel, n),
            out_shape=jax.ShapeDtypeStruct((own, d), BF16),
            in_specs=[hbm, vmem, vmem, hbm, hbm, hbm, hbm],
            out_specs=vmem,
            scratch_shapes=[
                pltpu.VMEM((own, d), BF16),
                pltpu.VMEM((own, d), F32),
                pltpu.VMEM((heads, own, HEAD), BF16),
                pltpu.VMEM((own, run * HEAD), BF16),
                pltpu.VMEM((kv_heads, n, 2 * own, HEAD), BF16),
                pltpu.VMEM((2, n * own, own), F32),
                pltpu.VMEM((2, 1, own), F32),
                pltpu.VMEM((own, HEAD), F32),
                pltpu.VMEM((own, HEAD), F32),
                pltpu.VMEM((SLOTS, d, WIDE), BF16),
                pltpu.SemaphoreType.DMA((SLOTS,)),
                pltpu.SemaphoreType.DMA,
                pltpu.SemaphoreType.DMA((2, kv_heads, n // 2)),
                pltpu.SemaphoreType.DMA((kv_heads, n)),
            ],
            compiler_params=pltpu.CompilerParams(collective_id=0, has_side_effects=True, vmem_limit_bytes=VMEM),
        )(x, gain[None], turn, wk, wv, wq, wo)

    tokens, whole = P(("dp", "sp"), None), P(None, None)
    return jax.shard_map(
        step,
        mesh=mesh,
        in_specs=(tokens, P(None), whole, whole, whole, whole),
        out_specs=tokens,
        check_vma=False,
    )
```
